32 devices in a mesh: tp: 8 (over z, y), dp: 4 (over x, core).
Axes of the slice: x: 2, y: 2, z: 4, core: 2. Of those that a mesh axis runs over, the one named last changes fastest.
Arguments:
- tokens: bfloat16 [32, 8192], P(None, ('dp', 'tp')), may hold values from -6 to 6
- query_weight: bfloat16 [8192, 8192], P('dp', 'tp'), may hold values from -0.0625 to 0.0625
- key_weight: bfloat16 [8192, 1024], P('dp', 'tp'), may hold values from -0.0625 to 0.0625
- value_weight: bfloat16 [8192, 1024], P('dp', 'tp'), may hold values from -0.0625 to 0.0625
- query_bias: bfloat16 [8192], P('tp'), may hold values from -3 to 3
- key_bias: bfloat16 [1024], P('tp'), may hold values from -6 to 6
- value_bias: bfloat16 [1024], P('tp'), may hold values from -6 to 6
- out_weight: bfloat16 [8192, 8192], P('tp', 'dp'), may hold values from -0.0625 to 0.0625
- key_pool: bfloat16 [2048, 16, 8, 128], P(('dp', 'tp')), may hold values from -12 to 12
- value_pool: bfloat16 [2048, 16, 8, 128], P(('dp', 'tp')), may hold values from -9 to 9
- page_table: int32 [32, 64], P('dp'), may hold values from 0 to 2047, as said below
- lengths: int32 [32], P('dp'), may hold values from 512 to 1023
Outputs:
- mixed: bfloat16 [32, 8192], P(None, ('dp', 'tp'))
- key_out: bfloat16 [2048, 16, 8, 128], P(('dp', 'tp'))
- value_out: bfloat16 [2048, 16, 8, 128], P(('dp', 'tp'))
The draws below stay inside these ranges and needn't reach their ends.
Inputs may be any that keep to these rules, and one draw needn't show every extreme that they name: page_table[b, j] is the pool page that holds positions 16 j to 16 j + 16 - 1 of sequence b; every page of the pool is named exactly once; page_table[b, j] // 64 equals (b // 8) * 8 + j % 8, so that page lies on the device of dp index b // 8 and tp index j % 8. lengths[b] is the position of sequence b's new token; positions 0 to lengths[b] - 1 of the cache hold earlier tokens.
All inputs are finite; a program needn't handle non-finite values.
Results may differ from the reference program's by a relative error of at most 0.007.
Values may be sent and summed in bfloat16 or wider, within the bound.
A program may use at most 64 MiB of HBM per device.

```python
import jax
import jax.numpy as jnp
from jax import lax

D = 8192
HEADS = 64
KV_HEADS = 8
HEAD_DIM = 128
PAGE = 16
SEQ_DEV = 8
PAGES_LOCAL = 8
BATCH = 32
SLOTS = 64
POOL = 2048
PAGES_SEQ = 64
CONTEXT = 1024


def shuffled(subkey):
    return jax.random.permutation(subkey, SLOTS)


def draw_page_table(key, part):
    tp_width = PAGES_SEQ // PAGES_LOCAL
    dp_width = BATCH // SEQ_DEV
    holders = dp_width * tp_width
    subkeys = jax.random.split(jax.random.fold_in(key, 7), holders)
    orders = jax.vmap(shuffled)(subkeys).astype(jnp.int32)
    blocks = orders + (jnp.arange(holders, dtype=jnp.int32) * SLOTS)[:, None]
    blocks = blocks.reshape(dp_width, tp_width, SEQ_DEV, PAGES_LOCAL)
    return jnp.transpose(blocks, (0, 2, 3, 1)).reshape(BATCH, PAGES_SEQ).astype(jnp.int32)


def with_ends(entries, rng, least, high):
    dims = entries.shape
    index_at = [jax.random.randint(jax.random.fold_in(rng, axis), (), 0, dims[axis]) for axis in range(len(dims))]
    entries = entries.at[tuple(index_at)].set(least)
    longest = dims.index(max(dims))
    index_at[longest] = (index_at[longest] + 1) % dims[longest]
    return entries.at[tuple(index_at)].set(high)


def levels(rng, dims, shards, smallest, top_value):
    gain, own = 1.0, jax.random.fold_in(rng, 6)
    for dim, parts in shards:
        draws = jnp.exp(jax.random.uniform(jax.random.fold_in(own, dim), (parts,), jnp.float32, smallest / len(shards), top_value / len(shards)))
        gain = gain * jnp.repeat(draws, dims[dim] // parts).reshape([-1 if axis == dim else 1 for axis in range(len(dims))])
    return gain


def bell_draw(stream_key, extent, spread, limit, pieces=(), held_as=jnp.bfloat16):
    entries = spread * jax.random.normal(stream_key, extent, jnp.float32)
    if pieces:
        entries = entries * levels(stream_key, extent, pieces, -0.22, 0.18)
    return jnp.clip(entries, -limit, limit).astype(held_as)


def setup_inputs(seed: int = 0) -> dict:
    keys = jax.random.split(jax.random.key(seed), 13)
    return {
        "tokens": bell_draw(keys[0], (BATCH, D), 1.0, 6.0, ((1, 32),)),
        "query_weight": bell_draw(keys[1], (D, HEADS * HEAD_DIM), D ** -0.5, 0.0625, ((0, 4), (1, 8))),
        "key_weight": bell_draw(keys[2], (D, KV_HEADS * HEAD_DIM), D ** -0.5, 0.0625, ((0, 4), (1, 8))),
        "value_weight": bell_draw(keys[3], (D, KV_HEADS * HEAD_DIM), D ** -0.5, 0.0625, ((0, 4), (1, 8))),
        "query_bias": bell_draw(keys[4], (HEADS * HEAD_DIM,), 0.5, 3.0, ((0, 8),)),
        "key_bias": bell_draw(keys[5], (KV_HEADS * HEAD_DIM,), 1.0, 6.0, ((0, 8),)),
        "value_bias": bell_draw(keys[6], (KV_HEADS * HEAD_DIM,), 1.0, 6.0, ((0, 8),)),
        "out_weight": bell_draw(keys[7], (HEADS * HEAD_DIM, D), (HEADS * HEAD_DIM) ** -0.5, 0.0625, ((0, 8), (1, 4))),
        "key_pool": bell_draw(keys[8], (POOL, PAGE, KV_HEADS, HEAD_DIM), 2.0, 12.0, ((0, 32),)),
        "value_pool": bell_draw(keys[9], (POOL, PAGE, KV_HEADS, HEAD_DIM), 1.5, 9.0, ((0, 32),)),
        "page_table": draw_page_table(jax.random.fold_in(keys[12], 71), 0),
        "lengths": with_ends(jax.random.randint(keys[11], (BATCH,), CONTEXT // 2, CONTEXT), jax.random.fold_in(keys[11], 1), CONTEXT // 2, CONTEXT - 1).astype(jnp.int32),
    }


rope_theta = 1000000.0
mask_value = -1.0e30


def rotate(vectors, position):
    head_width = vectors.shape[-1]
    half_width = head_width // 2
    frequency = rope_theta ** (-(jnp.arange(half_width, dtype=jnp.float32) * 2.0 / head_width))
    angles = position.astype(jnp.float32)[:, None] * frequency[None, :]
    cosine = jnp.cos(angles)[:, None, :]
    sine_part = jnp.sin(angles)[:, None, :]
    leading = vectors[..., :half_width]
    trailing = vectors[..., half_width:]
    return jnp.concatenate([leading * cosine - trailing * sine_part, trailing * cosine + leading * sine_part], axis=-1)


def reference(tokens, query_weight, key_weight, value_weight, query_bias, key_bias, value_bias, out_weight, key_pool, value_pool, page_table, lengths):
    query_lin = jnp.dot(tokens, query_weight, preferred_element_type=jnp.float32) + query_bias.astype(jnp.float32)
    key_lin = jnp.dot(tokens, key_weight, preferred_element_type=jnp.float32) + key_bias.astype(jnp.float32)
    value_lin = jnp.dot(tokens, value_weight, preferred_element_type=jnp.float32) + value_bias.astype(jnp.float32)
    query_rows = rotate(query_lin.reshape(BATCH, HEADS, HEAD_DIM), lengths).astype(jnp.bfloat16)
    new_key = rotate(key_lin.reshape(BATCH, KV_HEADS, HEAD_DIM), lengths).astype(jnp.bfloat16)
    new_value = value_lin.reshape(BATCH, KV_HEADS, HEAD_DIM).astype(jnp.bfloat16)
    sequence = jnp.arange(BATCH, dtype=jnp.int32)
    target = page_table[sequence, (lengths // PAGE).astype(jnp.int32)]
    offset = (lengths % PAGE).astype(jnp.int32)
    key_out = key_pool.at[target, offset].set(new_key)
    value_out = value_pool.at[target, offset].set(new_value)
    positions = jnp.arange(CONTEXT, dtype=jnp.int32)
    group_size = HEADS // KV_HEADS
    score_scale = HEAD_DIM ** -0.5

    def attend(inputs):
        head_query, page_ids, length = inputs
        key_rows = key_out[page_ids].reshape(CONTEXT, KV_HEADS, HEAD_DIM).astype(jnp.float32)
        value_rows = value_out[page_ids].reshape(CONTEXT, KV_HEADS, HEAD_DIM).astype(jnp.float32)
        grouped = head_query.reshape(KV_HEADS, group_size, HEAD_DIM).astype(jnp.float32)
        scores = jnp.einsum("gqd,sgd->gqs", grouped, key_rows, precision=lax.Precision.HIGHEST) * score_scale
        scores = jnp.where(positions[None, None, :] <= length, scores, mask_value)
        weights = jax.nn.softmax(scores, axis=-1)
        result = jnp.einsum("gqs,sgd->gqd", weights, value_rows, precision=lax.Precision.HIGHEST)
        return result.reshape(HEADS * HEAD_DIM).astype(jnp.bfloat16)

    attended = lax.map(attend, (query_rows, page_table, lengths))
    mixed = jnp.dot(attended, out_weight, preferred_element_type=jnp.float32).astype(jnp.bfloat16)
    return (mixed, key_out, value_out)
```

```python
import functools

import jax
import jax.numpy as jnp
from jax import lax
from jax.experimental import pallas as pl
from jax.experimental.pallas import tpu as pltpu
from jax.sharding import PartitionSpec as P

rope_theta = 1000000.0
mask_value = -1e30
MESH = pl.DeviceIdType.MESH
f32 = jnp.float32
bf16 = jnp.bfloat16


def lane_round(width):
    return -(-width // 128) * 128


def greet(tp, dp, me_tp, me_dp):
    barrier = pltpu.get_barrier_semaphore()
    for k in range(1, tp):
        pl.semaphore_signal(
            barrier, inc=1, device_id={"tp": lax.rem(me_tp + k, tp)}, device_id_type=MESH
        )
    for k in range(1, dp):
        pl.semaphore_signal(
            barrier, inc=1, device_id={"dp": lax.rem(me_dp + k, dp)}, device_id_type=MESH
        )
    pl.semaphore_wait(barrier, tp - 1 + dp - 1)


def remote(src, dst, send, recv, axis, peer):
    return pltpu.make_async_remote_copy(
        src_ref=src, dst_ref=dst, send_sem=send, recv_sem=recv,
        device_id={axis: peer}, device_id_type=MESH,
    )


def project_kernel(
    dims,
    tok_ref, wq_hbm, wk_hbm, wv_hbm, bq_ref, bk_ref, bv_ref, cs_ref,
    q_out, k_out, v_out,
    wq, wk, wv, tok, part, got, qsend, qgot, kvsend, kvgot,
    wsem, ts, tr, ps, pr, qs, qr, ks, kr,
):
    tp, dp, seq, head, lh, qcols, kcols, kpad = dims
    me, mdp = lax.axis_index("tp"), lax.axis_index("dp")
    width = tok_ref.shape[1]
    order = [lax.rem(me + k, tp) for k in range(tp)]
    wcopies = []
    for k in range(tp):
        t = lax.rem(me + tp - k, tp)
        rows = pl.ds(pl.multiple_of(t * width, width), width)
        c = pltpu.make_async_copy(wq_hbm.at[rows, :], wq.at[rows, :], wsem.at[k])
        c.start()
        wcopies.append(c)
        if k == 0:
            ck = pltpu.make_async_copy(wk_hbm, wk, wsem.at[tp])
            ck.start()
            cv = pltpu.make_async_copy(wv_hbm, wv, wsem.at[tp + 1])
            cv.start()
    greet(tp, dp, me, mdp)
    sends = []
    for k in range(1, tp):
        c = remote(tok_ref, tok.at[k], ts.at[k], tr.at[k], "tp", order[k])
        c.start()
        sends.append(c)
    accq = acck = accv = None
    for k in range(tp):
        t = lax.rem(me + tp - k, tp)
        rows = pl.ds(pl.multiple_of(t * width, width), width)
        wcopies[k].wait()
        if k == 0:
            ck.wait()
            cv.wait()
            block = tok_ref[...]
        else:
            sends[k - 1].wait_recv()
            block = tok[k]
        dq = jnp.dot(block, wq[rows, :], preferred_element_type=f32)
        dk = jnp.dot(block, wk[rows, :], preferred_element_type=f32)
        dv = jnp.dot(block, wv[rows, :], preferred_element_type=f32)
        if k == 0:
            accq, acck, accv = dq, dk, dv
        else:
            accq, acck, accv = accq + dq, acck + dk, accv + dv
    for d in range(dp):
        rs = slice(d * seq, (d + 1) * seq)
        part[d, :, 0:qcols] = accq[rs]
        part[d, :, qcols : qcols + kcols] = acck[rs]
        part[d, :, qcols + kpad : qcols + kpad + kcols] = accv[rs]
    psends = []
    for k in range(1, dp):
        d = lax.rem(mdp + k, dp)
        c = remote(part.at[d], got.at[k], ps.at[k], pr.at[k], "dp", d)
        c.start()
        psends.append(c)
    for c in psends:
        c.wait_recv()
    total = part[mdp]
    for k in range(1, dp):
        total = total + got[k]
    cosine, sine = cs_ref[0], cs_ref[1]
    klin = total[:, qcols : qcols + kcols] + bk_ref[...].astype(f32)
    vlin = total[:, qcols + kpad : qcols + kpad + kcols] + bv_ref[...].astype(f32)
    kvsend[0] = klin
    kvsend[1] = vlin
    for h in range(lh):
        hs = slice(h * head, (h + 1) * head)
        u = total[:, hs] + bq_ref[:, hs].astype(f32)
        r = u * cosine + pltpu.roll(u, head // 2, 1) * sine
        qsend[h * seq : (h + 1) * seq, :] = r.astype(bf16)
    qsends = []
    for k in range(1, tp):
        c = remote(qsend, qgot.at[k], qs.at[k], qr.at[k], "tp", order[k])
        c.start()
        c2 = remote(kvsend, kvgot.at[k], ks.at[k], kr.at[k], "tp", order[k])
        c2.start()
        qsends.append((c, c2))
    rows_dev = lh * seq

    def place(t, qv, kv, vv):
        q_out[t] = qv.astype(f32)
        k_out[t] = kv
        v_out[t] = vv

    place(me, qsend[...], klin, vlin)
    for k in range(1, tp):
        c, c2 = qsends[k - 1]
        c.wait_recv()
        c2.wait_recv()
        place(lax.rem(me + tp - k, tp), qgot[k], kvgot[k, 0], kvgot[k, 1])
    for c in sends + psends:
        c.wait_send()
    for c, c2 in qsends:
        c.wait_send()
        c2.wait_send()


def attend_kernel(
    dims,
    q_ref, kn_ref, vn_ref, cs_ref, table, lengths, kp_hbm, vp_hbm,
    ko_hbm, vo_hbm, o_out, st_out,
    kbuf, vbuf, krot, oscr, mscr, lscr, insem, outsem,
):
    tp, seq, heads, kvh, head, page, slots, pages, parts = dims
    me = lax.axis_index("tp")
    prow = page * kvh
    total_rows = slots * prow
    cut = total_rows // parts
    loads = []
    for i in range(parts):
        r = pl.ds(i * cut, cut)
        a = pltpu.make_async_copy(kp_hbm.at[r, :], kbuf.at[r, :], insem.at[0, i])
        a.start()
        loads.append(a)
    vloads = []
    for i in range(parts):
        r = pl.ds(i * cut, cut)
        a = pltpu.make_async_copy(vp_hbm.at[r, :], vbuf.at[r, :], insem.at[1, i])
        a.start()
        vloads.append(a)
    cosine, sine = cs_ref[0], cs_ref[1]
    for g in range(kvh):
        rs = slice(g * seq, (g + 1) * seq)
        u = kn_ref[rs, :]
        krot[rs, :] = u * cosine + pltpu.roll(u, head // 2, 1) * sine
    rowid = lax.broadcasted_iota(jnp.int32, (2 * kvh, head), 0) // kvh

    def patch(buf, src):
        for b in range(seq):
            length = lengths[b]
            where = length // page
            off = lax.rem(length, page)
            slot = lax.rem(table[b, where], slots)

            @pl.when(lax.rem(where, tp) == me)
            def _():
                base = pl.multiple_of(slot * prow + (off // 2) * (2 * kvh), 2 * kvh)
                fresh = src[pl.ds(b, kvh, stride=seq), :]
                fresh = jnp.concatenate([fresh, fresh], axis=0)
                old = buf[pl.ds(base, 2 * kvh), :].astype(f32)
                buf[pl.ds(base, 2 * kvh), :] = jnp.where(
                    rowid == lax.rem(off, 2), fresh, old
                ).astype(bf16)

    for a in loads:
        a.wait()
    patch(kbuf, krot)
    for a in vloads:
        a.wait()
    patch(vbuf, vn_ref)
    stores = []
    for i, (buf, out) in enumerate(((kbuf, ko_hbm), (vbuf, vo_hbm))):
        a = pltpu.make_async_copy(buf, out, outsem.at[i])
        a.start()
        stores.append(a)
    lane = lax.broadcasted_iota(jnp.int32, (heads, prow), 1)
    hrow = lax.broadcasted_iota(jnp.int32, (heads, prow), 0)
    same = lax.rem(lane, kvh) == hrow // (heads // kvh)
    step = lane // kvh
    scale = head ** (-0.5)
    for b in range(seq):
        length = lengths[b]
        qb = q_ref[pl.ds(b, heads, stride=seq), :].astype(bf16)
        scores, rows = [], []
        for j in range(pages):
            slot = lax.rem(table[b, j * tp + me], slots)
            r = pl.ds(pl.multiple_of(slot * prow, prow), prow)
            rows.append(r)
            s = lax.dot_general(
                qb, kbuf[r, :], (((1,), (1,)), ((), ())), preferred_element_type=f32
            )
            first = (j * tp + me) * page
            scores.append(jnp.where(same & (step <= length - first), s * scale, mask_value))
        peak = functools.reduce(jnp.maximum, scores)
        peak = jnp.max(peak, axis=1, keepdims=True)
        acc = None
        tot = None
        for j in range(pages):
            p = jnp.exp(scores[j] - peak).astype(bf16)
            d = jnp.dot(p, vbuf[rows[j], :], preferred_element_type=f32)
            acc = d if acc is None else acc + d
            pf = p.astype(f32)
            tot = pf if tot is None else tot + pf
        tot = jnp.sum(tot, axis=1, keepdims=True)
        dst = pl.ds(b, heads, stride=seq)
        oscr[dst, :] = acc
        mscr[dst, :] = jnp.broadcast_to(peak, (heads, head))
        lscr[dst, :] = jnp.broadcast_to(tot, (heads, head))
    block = heads // tp * seq
    row = lax.broadcasted_iota(jnp.int32, (block, head), 0)
    col = lax.broadcasted_iota(jnp.int32, (block, head), 1)
    for t in range(tp):
        r = slice(t * block, (t + 1) * block)
        o_out[t] = oscr[r, :].astype(bf16)
        line = jnp.where(col == row, mscr[r, :], 0.0)
        line = line + jnp.where(col == row + block, lscr[r, :], 0.0)
        line = jnp.sum(line, axis=0, keepdims=True)
        st_out[t] = jnp.broadcast_to(line, (8, head))
    for a in stores:
        a.wait()


def mix_kernel(
    dims,
    o_ref, st_ref, w_hbm, out_ref,
    w, og, sg, att, attg, psend, pgot,
    wsem, os, orr, ss, sr, as_, ar, ps, pr,
):
    tp, dp, seq, head, lh, width = dims
    me, mdp = lax.axis_index("tp"), lax.axis_index("dp")
    block = lh * seq
    wc = pltpu.make_async_copy(w_hbm, w, wsem.at[0])
    wc.start()
    greet(tp, dp, me, mdp)
    sends = []
    for k in range(1, tp):
        t = lax.rem(me + k, tp)
        c2 = remote(st_ref.at[t], sg.at[k], ss.at[k], sr.at[k], "tp", t)
        c2.start()
        c = remote(o_ref.at[t], og.at[k], os.at[k], orr.at[k], "tp", t)
        c.start()
        sends.append((c, c2))
    row = lax.broadcasted_iota(jnp.int32, (block, head), 0)
    col = lax.broadcasted_iota(jnp.int32, (block, head), 1)

    def column(line, shift):
        return jnp.sum(jnp.where(col == row + shift, line, 0.0), axis=1, keepdims=True)

    peaks, totals = [], []
    for k in range(tp):
        if k:
            sends[k - 1][1].wait_recv()
            line = sg[k, 0:1, :]
        else:
            line = st_ref[me, 0:1, :]
        peaks.append(column(line, 0))
        totals.append(column(line, block))
    highest = functools.reduce(jnp.maximum, peaks)
    acc = tot = None
    for k in range(tp):
        if k:
            sends[k - 1][0].wait_recv()
            o = og[k]
        else:
            o = o_ref[me]
        fac = jnp.exp(peaks[k] - highest)
        a = o.astype(f32) * fac
        l = totals[k] * fac
        acc = a if acc is None else acc + a
        tot = l if tot is None else tot + l
    res = acc / tot
    for h in range(lh):
        att[:, h * head : (h + 1) * head] = res[h * seq : (h + 1) * seq, :].astype(bf16)
    asends = []
    for k in range(1, dp):
        d = lax.rem(mdp + k, dp)
        c = remote(att, attg.at[mdp], as_.at[k], ar.at[k], "dp", d)
        c.start()
        asends.append(c)
    attg[mdp] = att[...]
    for c in asends:
        c.wait_recv()
    rows = jnp.concatenate([attg[d].astype(f32) for d in range(dp)], axis=0).astype(bf16)
    wc.wait()
    aligned = width % 128 == 0
    if not aligned:
        for t in range(tp):
            ws = w[:, t * width : (t + 1) * width]
            psend[t] = jnp.dot(rows, ws, preferred_element_type=f32).astype(bf16)

    def product(t):
        ws = w[:, pl.ds(pl.multiple_of(t * width, width), width)]
        return jnp.dot(rows, ws, preferred_element_type=f32)

    psends = []
    for k in range(1, tp):
        t = lax.rem(me + k, tp)
        if aligned:
            psend[t] = product(t).astype(bf16)
        c = remote(psend.at[t], pgot.at[k], ps.at[k], pr.at[k], "tp", t)
        c.start()
        psends.append(c)
    total = product(me) if aligned else psend[me].astype(f32)
    for k in range(1, tp):
        psends[k - 1].wait_recv()
        total = total + pgot[k].astype(f32)
    out_ref[...] = total.astype(bf16)
    for c, c2 in sends:
        c.wait_send()
        c2.wait_send()
    for c in asends + psends:
        c.wait_send()


def local(
    tokens, query_weight, key_weight, value_weight, query_bias, key_bias, value_bias,
    out_weight, key_pool, value_pool, page_table, lengths,
):
    tp, dp = lax.axis_size("tp"), lax.axis_size("dp")
    seq = page_table.shape[0]
    slots, page, kvh, head = key_pool.shape
    depth, qcols = query_weight.shape
    kcols = key_weight.shape[1]
    kpad = lane_round(kcols)
    lh = qcols // head
    heads = lh * tp
    batch, width = tokens.shape
    pages = page_table.shape[1] // tp
    block = lh * seq
    half = head // 2
    frequency = rope_theta ** (-(jnp.arange(half, dtype=f32) * 2.0 / head))
    angles = lengths.astype(f32)[:, None] * frequency[None, :]
    cosine, sine = jnp.cos(angles), jnp.sin(angles)
    cs = jnp.stack(
        [jnp.concatenate([cosine, cosine], 1), jnp.concatenate([-sine, sine], 1)]
    )
    vm = pl.BlockSpec(memory_space=pltpu.VMEM)
    hbm = pl.BlockSpec(memory_space=pltpu.HBM)
    sm = pl.BlockSpec(memory_space=pltpu.SMEM)
    dma = pltpu.SemaphoreType.DMA
    q, kn, vn = pl.pallas_call(
        functools.partial(project_kernel, (tp, dp, seq, head, lh, qcols, kcols, kpad)),
        out_shape=(
            jax.ShapeDtypeStruct((tp, block, head), f32),
            jax.ShapeDtypeStruct((tp, seq, kcols), f32),
            jax.ShapeDtypeStruct((tp, seq, kcols), f32),
        ),
        in_specs=[vm, hbm, hbm, hbm, vm, vm, vm, vm],
        out_specs=(vm, vm, vm),
        scratch_shapes=[
            pltpu.VMEM((depth, qcols), bf16),
            pltpu.VMEM((depth, kcols), bf16),
            pltpu.VMEM((depth, kcols), bf16),
            pltpu.VMEM((tp, batch, width), bf16),
            pltpu.VMEM((dp, seq, qcols + 2 * kpad), f32),
            pltpu.VMEM((dp, seq, qcols + 2 * kpad), f32),
            pltpu.VMEM((block, head), bf16),
            pltpu.VMEM((tp, block, head), bf16),
            pltpu.VMEM((2, seq, kcols), f32),
            pltpu.VMEM((tp, 2, seq, kcols), f32),
            dma((tp + 2,)),
            dma((tp,)), dma((tp,)), dma((dp,)), dma((dp,)),
            dma((tp,)), dma((tp,)), dma((tp,)), dma((tp,)),
        ],
        compiler_params=pltpu.CompilerParams(
            collective_id=0, has_side_effects=True, vmem_limit_bytes=24 * 2**20
        ),
        name="project",
    )(
        tokens, query_weight, key_weight, value_weight,
        query_bias[None], key_bias[None], value_bias[None], cs,
    )
    if kcols != head:
        kn = kn.transpose(1, 0, 2).reshape(seq, kvh, head).transpose(1, 0, 2)
        vn = vn.transpose(1, 0, 2).reshape(seq, kvh, head).transpose(1, 0, 2)
    rows = slots * page * kvh
    parts = 4
    ko, vo, o, st = pl.pallas_call(
        functools.partial(
            attend_kernel, (tp, seq, heads, kvh, head, page, slots, pages, parts)
        ),
        out_shape=(
            jax.ShapeDtypeStruct((rows, head), bf16),
            jax.ShapeDtypeStruct((rows, head), bf16),
            jax.ShapeDtypeStruct((tp, block, head), bf16),
            jax.ShapeDtypeStruct((tp, 8, head), f32),
        ),
        in_specs=[vm, vm, vm, vm, sm, sm, hbm, hbm],
        out_specs=(hbm, hbm, vm, vm),
        scratch_shapes=[
            pltpu.VMEM((rows, head), bf16),
            pltpu.VMEM((rows, head), bf16),
            pltpu.VMEM((kvh * seq, head), f32),
            pltpu.VMEM((heads * seq, head), f32),
            pltpu.VMEM((heads * seq, head), f32),
            pltpu.VMEM((heads * seq, head), f32),
            dma((2, parts)),
            dma((2,)),
        ],
        compiler_params=pltpu.CompilerParams(vmem_limit_bytes=24 * 2**20),
        name="attend",
    )(
        q.reshape(heads * seq, head), kn.reshape(kvh * seq, head), vn.reshape(kvh * seq, head),
        cs, page_table, lengths,
        key_pool.reshape(rows, head), value_pool.reshape(rows, head),
    )
    out_width = out_weight.shape[1] // tp
    mixed = pl.pallas_call(
        functools.partial(mix_kernel, (tp, dp, seq, head, lh, out_width)),
        out_shape=jax.ShapeDtypeStruct((batch, out_width), bf16),
        in_specs=[vm, vm, hbm],
        out_specs=vm,
        scratch_shapes=[
            pltpu.VMEM(out_weight.shape, bf16),
            pltpu.VMEM((tp, block, head), bf16),
            pltpu.VMEM((tp, 8, head), f32),
            pltpu.VMEM((seq, qcols), bf16),
            pltpu.VMEM((dp, seq, qcols), bf16),
            pltpu.VMEM((tp, batch, out_width), bf16),
            pltpu.VMEM((tp, batch, out_width), bf16),
            dma((1,)),
            dma((tp,)), dma((tp,)), dma((tp,)), dma((tp,)),
            dma((dp,)), dma((dp,)), dma((tp,)), dma((tp,)),
        ],
        compiler_params=pltpu.CompilerParams(
            collective_id=1, has_side_effects=True, vmem_limit_bytes=24 * 2**20
        ),
        name="mix",
    )(o, st, out_weight)
    return mixed, ko.reshape(key_pool.shape), vo.reshape(value_pool.shape)


def solution(mesh):
    in_specs = (
        P(None, ("dp", "tp")),
        P("dp", "tp"),
        P("dp", "tp"),
        P("dp", "tp"),
        P("tp"),
        P("tp"),
        P("tp"),
        P("tp", "dp"),
        P(("dp", "tp"), None, None, None),
        P(("dp", "tp"), None, None, None),
        P("dp", None),
        P("dp"),
    )
    out_specs = (
        P(None, ("dp", "tp")),
        P(("dp", "tp"), None, None, None),
        P(("dp", "tp"), None, None, None),
    )
    return jax.shard_map(local, mesh=mesh, in_specs=in_specs, out_specs=out_specs, check_vma=False)
```

```python
import functools

import jax
import jax.numpy as jnp
from jax import lax
from jax.experimental import pallas as pl
from jax.experimental.pallas import tpu as pltpu
from jax.sharding import PartitionSpec as P

rope_theta = 1000000.0
mask_value = -1e30
MESH = pl.DeviceIdType.MESH
f32 = jnp.float32
bf16 = jnp.bfloat16


def lane_round(width):
    return -(-width // 128) * 128


def greet(tp, dp, me_tp, me_dp):
    barrier = pltpu.get_barrier_semaphore()
    for k in range(1, tp):
        pl.semaphore_signal(
            barrier, inc=1, device_id={"tp": lax.rem(me_tp + k, tp)}, device_id_type=MESH
        )
    for k in range(1, dp):
        pl.semaphore_signal(
            barrier, inc=1, device_id={"dp": lax.rem(me_dp + k, dp)}, device_id_type=MESH
        )
    pl.semaphore_wait(barrier, tp - 1 + dp - 1)


def remote(src, dst, send, recv, axis, peer):
    return pltpu.make_async_remote_copy(
        src_ref=src, dst_ref=dst, send_sem=send, recv_sem=recv,
        device_id={axis: peer}, device_id_type=MESH,
    )


def project_kernel(
    dims,
    tok_ref, wq_hbm, wk_hbm, wv_hbm, bq_ref, bk_ref, bv_ref, cs_ref,
    q_out, k_out, v_out,
    wq, wk, wv, tok, part, got, qsend, qgot, kvsend, kvgot,
    wsem, ts, tr, ps, pr, qs, qr, ks, kr,
):
    tp, dp, seq, head, lh, qcols, kcols, kpad = dims
    me, mdp = lax.axis_index("tp"), lax.axis_index("dp")
    width = tok_ref.shape[1]
    order = [lax.rem(me + k, tp) for k in range(tp)]
    wcopies = []
    for k in range(tp):
        t = lax.rem(me + tp - k, tp)
        rows = pl.ds(pl.multiple_of(t * width, width), width)
        c = pltpu.make_async_copy(wq_hbm.at[rows, :], wq.at[rows, :], wsem.at[k])
        c.start()
        wcopies.append(c)
        if k == 0:
            ck = pltpu.make_async_copy(wk_hbm, wk, wsem.at[tp])
            ck.start()
            cv = pltpu.make_async_copy(wv_hbm, wv, wsem.at[tp + 1])
            cv.start()
    greet(tp, dp, me, mdp)
    sends = []
    for k in range(1, tp):
        c = remote(tok_ref, tok.at[k], ts.at[k], tr.at[k], "tp", order[k])
        c.start()
        sends.append(c)
    accq = acck = accv = None
    for k in range(tp):
        t = lax.rem(me + tp - k, tp)
        rows = pl.ds(pl.multiple_of(t * width, width), width)
        wcopies[k].wait()
        if k == 0:
            ck.wait()
            cv.wait()
            block = tok_ref[...]
        else:
            sends[k - 1].wait_recv()
            block = tok[k]
        dq = jnp.dot(block, wq[rows, :], preferred_element_type=f32)
        dk = jnp.dot(block, wk[rows, :], preferred_element_type=f32)
        dv = jnp.dot(block, wv[rows, :], preferred_element_type=f32)
        if k == 0:
            accq, acck, accv = dq, dk, dv
        else:
            accq, acck, accv = accq + dq, acck + dk, accv + dv
    for d in range(dp):
        rs = slice(d * seq, (d + 1) * seq)
        part[d, :, 0:qcols] = accq[rs]
        part[d, :, qcols : qcols + kcols] = acck[rs]
        part[d, :, qcols + kpad : qcols + kpad + kcols] = accv[rs]
    psends = []
    for k in range(1, dp):
        d = lax.rem(mdp + k, dp)
        c = remote(part.at[d], got.at[k], ps.at[k], pr.at[k], "dp", d)
        c.start()
        psends.append(c)
    for c in psends:
        c.wait_recv()
    total = part[mdp]
    for k in range(1, dp):
        total = total + got[k]
    cosine, sine = cs_ref[0], cs_ref[1]
    klin = total[:, qcols : qcols + kcols] + bk_ref[...].astype(f32)
    vlin = total[:, qcols + kpad : qcols + kpad + kcols] + bv_ref[...].astype(f32)
    kvsend[0] = klin
    kvsend[1] = vlin
    for h in range(lh):
        hs = slice(h * head, (h + 1) * head)
        u = total[:, hs] + bq_ref[:, hs].astype(f32)
        r = u * cosine + pltpu.roll(u, head // 2, 1) * sine
        qsend[h * seq : (h + 1) * seq, :] = r.astype(bf16)
    qsends = []
    for k in range(1, tp):
        c = remote(qsend, qgot.at[k], qs.at[k], qr.at[k], "tp", order[k])
        c.start()
        c2 = remote(kvsend, kvgot.at[k], ks.at[k], kr.at[k], "tp", order[k])
        c2.start()
        qsends.append((c, c2))
    rows_dev = lh * seq

    def place(t, qv, kv, vv):
        q_out[t] = qv.astype(f32)
        k_out[t] = kv
        v_out[t] = vv

    place(me, qsend[...], klin, vlin)
    for k in range(1, tp):
        c, c2 = qsends[k - 1]
        c.wait_recv()
        c2.wait_recv()
        place(lax.rem(me + tp - k, tp), qgot[k], kvgot[k, 0], kvgot[k, 1])
    for c in sends + psends:
        c.wait_send()
    for c, c2 in qsends:
        c.wait_send()
        c2.wait_send()


def attend_kernel(
    dims,
    q_ref, kn_ref, vn_ref, cs_ref, table, lengths, kp_hbm, vp_hbm,
    ko_hbm, vo_hbm, o_out, st_out,
    kbuf, vbuf, krot, oscr, mscr, lscr, insem, outsem,
):
    tp, seq, heads, kvh, head, page, slots, pages, parts = dims
    me = lax.axis_index("tp")
    prow = page * kvh
    total_rows = slots * prow
    cut = total_rows // parts
    loads = []
    for i in range(parts):
        r = pl.ds(i * cut, cut)
        a = pltpu.make_async_copy(kp_hbm.at[r, :], kbuf.at[r, :], insem.at[0, i])
        a.start()
        loads.append(a)
    vloads = []
    for i in range(parts):
        r = pl.ds(i * cut, cut)
        a = pltpu.make_async_copy(vp_hbm.at[r, :], vbuf.at[r, :], insem.at[1, i])
        a.start()
        vloads.append(a)
    cosine, sine = cs_ref[0], cs_ref[1]
    for g in range(kvh):
        rs = slice(g * seq, (g + 1) * seq)
        u = kn_ref[rs, :]
        krot[rs, :] = u * cosine + pltpu.roll(u, head // 2, 1) * sine
    rowid = lax.broadcasted_iota(jnp.int32, (2 * kvh, head), 0) // kvh

    def patch(buf, src):
        for b in range(seq):
            length = lengths[b]
            where = length // page
            off = lax.rem(length, page)
            slot = lax.rem(table[b, where], slots)

            @pl.when(lax.rem(where, tp) == me)
            def _():
                base = pl.multiple_of(slot * prow + (off // 2) * (2 * kvh), 2 * kvh)
                fresh = src[pl.ds(b, kvh, stride=seq), :]
                fresh = jnp.concatenate([fresh, fresh], axis=0)
                old = buf[pl.ds(base, 2 * kvh), :].astype(f32)
                buf[pl.ds(base, 2 * kvh), :] = jnp.where(
                    rowid == lax.rem(off, 2), fresh, old
                ).astype(bf16)

    for a in loads:
        a.wait()
    patch(kbuf, krot)
    for a in vloads:
        a.wait()
    patch(vbuf, vn_ref)
    stores = []
    for i, (buf, out) in enumerate(((kbuf, ko_hbm), (vbuf, vo_hbm))):
        a = pltpu.make_async_copy(buf, out, outsem.at[i])
        a.start()
        stores.append(a)
    lane = lax.broadcasted_iota(jnp.int32, (heads, prow), 1)
    hrow = lax.broadcasted_iota(jnp.int32, (heads, prow), 0)
    same = lax.rem(lane, kvh) == hrow // (heads // kvh)
    step = lane // kvh
    scale = head ** (-0.5)
    for b in range(seq):
        length = lengths[b]
        qb = q_ref[pl.ds(b, heads, stride=seq), :].astype(bf16)
        scores, rows = [], []
        for j in range(pages):
            slot = lax.rem(table[b, j * tp + me], slots)
            r = pl.ds(pl.multiple_of(slot * prow, prow), prow)
            rows.append(r)
            s = lax.dot_general(
                qb, kbuf[r, :], (((1,), (1,)), ((), ())), preferred_element_type=f32
            )
            first = (j * tp + me) * page
            scores.append(jnp.where(same & (step <= length - first), s * scale, mask_value))
        peak = functools.reduce(jnp.maximum, scores)
        peak = jnp.max(peak, axis=1, keepdims=True)
        acc = None
        tot = None
        for j in range(pages):
            p = jnp.exp(scores[j] - peak).astype(bf16)
            d = jnp.dot(p, vbuf[rows[j], :], preferred_element_type=f32)
            acc = d if acc is None else acc + d
            pf = p.astype(f32)
            tot = pf if tot is None else tot + pf
        tot = jnp.sum(tot, axis=1, keepdims=True)
        dst = pl.ds(b, heads, stride=seq)
        oscr[dst, :] = acc
        mscr[dst, :] = jnp.broadcast_to(peak, (heads, head))
        lscr[dst, :] = jnp.broadcast_to(tot, (heads, head))
    block = heads // tp * seq
    row = lax.broadcasted_iota(jnp.int32, (block, head), 0)
    col = lax.broadcasted_iota(jnp.int32, (block, head), 1)
    for t in range(tp):
        r = slice(t * block, (t + 1) * block)
        o_out[t] = oscr[r, :].astype(bf16)
        line = jnp.where(col == row, mscr[r, :], 0.0)
        line = line + jnp.where(col == row + block, lscr[r, :], 0.0)
        line = jnp.sum(line, axis=0, keepdims=True)
        st_out[t] = jnp.broadcast_to(line, (8, head))
    for a in stores:
        a.wait()


def mix_kernel(
    dims,
    o_ref, st_ref, w_hbm, out_ref,
    w, og, sg, att, attg, psend, pgot,
    wsem, os, orr, ss, sr, as_, ar, ps, pr,
):
    tp, dp, seq, head, lh, width = dims
    me, mdp = lax.axis_index("tp"), lax.axis_index("dp")
    block = lh * seq
    wc = pltpu.make_async_copy(w_hbm, w, wsem.at[0])
    wc.start()
    greet(tp, dp, me, mdp)
    sends = []
    for k in range(1, tp):
        t = lax.rem(me + k, tp)
        c2 = remote(st_ref.at[t], sg.at[k], ss.at[k], sr.at[k], "tp", t)
        c2.start()
        c = remote(o_ref.at[t], og.at[k], os.at[k], orr.at[k], "tp", t)
        c.start()
        sends.append((c, c2))
    row = lax.broadcasted_iota(jnp.int32, (block, head), 0)
    col = lax.broadcasted_iota(jnp.int32, (block, head), 1)

    def column(line, shift):
        return jnp.sum(jnp.where(col == row + shift, line, 0.0), axis=1, keepdims=True)

    peaks, totals = [], []
    for k in range(tp):
        if k:
            sends[k - 1][1].wait_recv()
            line = sg[k, 0:1, :]
        else:
            line = st_ref[me, 0:1, :]
        peaks.append(column(line, 0))
        totals.append(column(line, block))
    highest = functools.reduce(jnp.maximum, peaks)
    acc = tot = None
    for k in range(tp):
        if k:
            sends[k - 1][0].wait_recv()
            o = og[k]
        else:
            o = o_ref[me]
        fac = jnp.exp(peaks[k] - highest)
        a = o.astype(f32) * fac
        l = totals[k] * fac
        acc = a if acc is None else acc + a
        tot = l if tot is None else tot + l
    res = acc / tot
    for h in range(lh):
        att[:, h * head : (h + 1) * head] = res[h * seq : (h + 1) * seq, :].astype(bf16)
    asends = []
    for k in range(1, dp):
        d = lax.rem(mdp + k, dp)
        c = remote(att, attg.at[mdp], as_.at[k], ar.at[k], "dp", d)
        c.start()
        asends.append(c)
    attg[mdp] = att[...]
    for c in asends:
        c.wait_recv()
    rows = jnp.concatenate([attg[d].astype(f32) for d in range(dp)], axis=0).astype(bf16)
    wc.wait()
    aligned = width % 128 == 0
    if not aligned:
        for t in range(tp):
            ws = w[:, t * width : (t + 1) * width]
            psend[t] = jnp.dot(rows, ws, preferred_element_type=f32).astype(bf16)

    def product(t):
        ws = w[:, pl.ds(pl.multiple_of(t * width, width), width)]
        return jnp.dot(rows, ws, preferred_element_type=f32)

    psends = []
    for k in range(1, tp):
        t = lax.rem(me + k, tp)
        if aligned:
            psend[t] = product(t).astype(bf16)
        c = remote(psend.at[t], pgot.at[k], ps.at[k], pr.at[k], "tp", t)
        c.start()
        psends.append(c)
    total = product(me) if aligned else psend[me].astype(f32)
    for k in range(1, tp):
        psends[k - 1].wait_recv()
        total = total + pgot[k].astype(f32)
    out_ref[...] = total.astype(bf16)
    for c, c2 in sends:
        c.wait_send()
        c2.wait_send()
    for c in asends + psends:
        c.wait_send()


def local(
    tokens, query_weight, key_weight, value_weight, query_bias, key_bias, value_bias,
    out_weight, key_pool, value_pool, page_table, lengths,
):
    tp, dp = lax.axis_size("tp"), lax.axis_size("dp")
    seq = page_table.shape[0]
    slots, page, kvh, head = key_pool.shape
    depth, qcols = query_weight.shape
    kcols = key_weight.shape[1]
    kpad = lane_round(kcols)
    lh = qcols // head
    heads = lh * tp
    batch, width = tokens.shape
    pages = page_table.shape[1] // tp
    block = lh * seq
    half = head // 2
    frequency = rope_theta ** (-(jnp.arange(half, dtype=f32) * 2.0 / head))
    angles = lengths.astype(f32)[:, None] * frequency[None, :]
    cosine, sine = jnp.cos(angles), jnp.sin(angles)
    cs = jnp.stack(
        [jnp.concatenate([cosine, cosine], 1), jnp.concatenate([-sine, sine], 1)]
    )
    vm = pl.BlockSpec(memory_space=pltpu.VMEM)
    hbm = pl.BlockSpec(memory_space=pltpu.HBM)
    sm = pl.BlockSpec(memory_space=pltpu.SMEM)
    dma = pltpu.SemaphoreType.DMA
    q, kn, vn = pl.pallas_call(
        functools.partial(project_kernel, (tp, dp, seq, head, lh, qcols, kcols, kpad)),
        out_shape=(
            jax.ShapeDtypeStruct((tp, block, head), f32),
            jax.ShapeDtypeStruct((tp, seq, kcols), f32),
            jax.ShapeDtypeStruct((tp, seq, kcols), f32),
        ),
        in_specs=[vm, hbm, hbm, hbm, vm, vm, vm, vm],
        out_specs=(vm, vm, vm),
        scratch_shapes=[
            pltpu.VMEM((depth, qcols), bf16),
            pltpu.VMEM((depth, kcols), bf16),
            pltpu.VMEM((depth, kcols), bf16),
            pltpu.VMEM((tp, batch, width), bf16),
            pltpu.VMEM((dp, seq, qcols + 2 * kpad), f32),
            pltpu.VMEM((dp, seq, qcols + 2 * kpad), f32),
            pltpu.VMEM((block, head), bf16),
            pltpu.VMEM((tp, block, head), bf16),
            pltpu.VMEM((2, seq, kcols), f32),
            pltpu.VMEM((tp, 2, seq, kcols), f32),
            dma((tp + 2,)),
            dma((tp,)), dma((tp,)), dma((dp,)), dma((dp,)),
            dma((tp,)), dma((tp,)), dma((tp,)), dma((tp,)),
        ],
        compiler_params=pltpu.CompilerParams(
            collective_id=0, has_side_effects=True
        ),
        name="project",
    )(
        tokens, query_weight, key_weight, value_weight,
        query_bias[None], key_bias[None], value_bias[None], cs,
    )
    if kcols != head:
        kn = kn.transpose(1, 0, 2).reshape(seq, kvh, head).transpose(1, 0, 2)
        vn = vn.transpose(1, 0, 2).reshape(seq, kvh, head).transpose(1, 0, 2)
    rows = slots * page * kvh
    parts = 4
    ko, vo, o, st = pl.pallas_call(
        functools.partial(
            attend_kernel, (tp, seq, heads, kvh, head, page, slots, pages, parts)
        ),
        out_shape=(
            jax.ShapeDtypeStruct((rows, head), bf16),
            jax.ShapeDtypeStruct((rows, head), bf16),
            jax.ShapeDtypeStruct((tp, block, head), bf16),
            jax.ShapeDtypeStruct((tp, 8, head), f32),
        ),
        in_specs=[vm, vm, vm, vm, sm, sm, hbm, hbm],
        out_specs=(hbm, hbm, vm, vm),
        scratch_shapes=[
            pltpu.VMEM((rows, head), bf16),
            pltpu.VMEM((rows, head), bf16),
            pltpu.VMEM((kvh * seq, head), f32),
            pltpu.VMEM((heads * seq, head), f32),
            pltpu.VMEM((heads * seq, head), f32),
            pltpu.VMEM((heads * seq, head), f32),
            dma((2, parts)),
            dma((2,)),
        ],
        name="attend",
    )(
        q.reshape(heads * seq, head), kn.reshape(kvh * seq, head), vn.reshape(kvh * seq, head),
        cs, page_table, lengths,
        key_pool.reshape(rows, head), value_pool.reshape(rows, head),
    )
    out_width = out_weight.shape[1] // tp
    mixed = pl.pallas_call(
        functools.partial(mix_kernel, (tp, dp, seq, head, lh, out_width)),
        out_shape=jax.ShapeDtypeStruct((batch, out_width), bf16),
        in_specs=[vm, vm, hbm],
        out_specs=vm,
        scratch_shapes=[
            pltpu.VMEM(out_weight.shape, bf16),
            pltpu.VMEM((tp, block, head), bf16),
            pltpu.VMEM((tp, 8, head), f32),
            pltpu.VMEM((seq, qcols), bf16),
            pltpu.VMEM((dp, seq, qcols), bf16),
            pltpu.VMEM((tp, batch, out_width), bf16),
            pltpu.VMEM((tp, batch, out_width), bf16),
            dma((1,)),
            dma((tp,)), dma((tp,)), dma((tp,)), dma((tp,)),
            dma((dp,)), dma((dp,)), dma((tp,)), dma((tp,)),
        ],
        compiler_params=pltpu.CompilerParams(
            collective_id=1, has_side_effects=True
        ),
        name="mix",
    )(o, st, out_weight)
    return mixed, ko.reshape(key_pool.shape), vo.reshape(value_pool.shape)


def solution(mesh):
    in_specs = (
        P(None, ("dp", "tp")),
        P("dp", "tp"),
        P("dp", "tp"),
        P("dp", "tp"),
        P("tp"),
        P("tp"),
        P("tp"),
        P("tp", "dp"),
        P(("dp", "tp"), None, None, None),
        P(("dp", "tp"), None, None, None),
        P("dp", None),
        P("dp"),
    )
    out_specs = (
        P(None, ("dp", "tp")),
        P(("dp", "tp"), None, None, None),
        P(("dp", "tp"), None, None, None),
    )
    return jax.shard_map(local, mesh=mesh, in_specs=in_specs, out_specs=out_specs, check_vma=False)
```
